128 devices in a mesh: patch: 32 (over y, z, core), hidden: 4 (over x).
Axes of the slice: x: 4, y: 4, z: 4, core: 2. Of those that a mesh axis runs over, the one named last changes fastest.
Arguments:
- nodes: bfloat16 [65536, 512], P('patch', 'hidden'), may hold values from -6 to 6
- edges: bfloat16 [262144, 512], P(('patch', 'hidden')), may hold values from -6 to 6
- senders: int32 [262144], P(('patch', 'hidden')), may hold values from 0 to 4351
- receivers: int32 [262144], P(('patch', 'hidden')), may hold values from 0 to 2047
- halo_rows: int32 [32, 2, 1024], P('patch'), may hold values from 0 to 2047
- coarse_rows: int32 [32, 32, 8], P('patch'), may hold values from 0 to 63
- edge_count: int32 [128], P(('patch', 'hidden')), may hold values from 1024 to 2048, as said below
- w_edge_in: bfloat16 [1536, 512], replicated, may hold values from -0.15625 to 0.15625
- b_edge_in: float32 [512], replicated, may hold values from -3 to 3
- w_edge_out: bfloat16 [512, 512], replicated, may hold values from -0.25 to 0.25
- b_edge_out: float32 [512], replicated, may hold values from -2 to 2
- edge_gain: float32 [512], replicated, may hold values from 0.5 to 1.5
- edge_shift: float32 [512], replicated, may hold values from -1 to 1
- w_node_in: bfloat16 [1024, 512], replicated, may hold values from -0.1875 to 0.1875
- b_node_in: float32 [512], replicated, may hold values from -3 to 3
- w_node_out: bfloat16 [512, 512], replicated, may hold values from -0.25 to 0.25
- b_node_out: float32 [512], replicated, may hold values from -2 to 2
- node_gain: float32 [512], replicated, may hold values from 0.5 to 1.5
- node_shift: float32 [512], replicated, may hold values from -1 to 1
Outputs:
- nodes_out: bfloat16 [65536, 512], P('patch', 'hidden')
- edges_out: bfloat16 [262144, 512], P(('patch', 'hidden'))
The draws below stay inside these ranges and needn't reach their ends.
Inputs may be any that keep to these rules, and one draw needn't show every extreme that they name: `edge_count`: some block holds 2048 live edges.
All inputs are finite; a program needn't handle non-finite values.
Results may differ from the reference program's by a relative error of at most 0.007.
Values may be sent and summed in bfloat16 or wider, within the bound.
No kernel may reach another device: no remote copies, remote signals or barrier semaphores. Data moves between devices by JAX's collectives and lax.ppermute only.
A program may use at most 128 MiB of HBM per device.

```python
import jax
import jax.numpy as jnp
from jax import lax

D = 512
NODE_DEV = 2048
EDGE_DEV = 2048
COARSE_DEV = 64
SLOT = 8
HALO = 1024
PATCHES = 32
SHARDS = 128
NODES = 65536
EDGES = 262144
TABLE = 4352
N_HIDDEN = 4


def draw_edge_count(key, part):
    draw_key, pick_key = jax.random.split(jax.random.fold_in(key, 11))
    counts = jax.random.randint(draw_key, (SHARDS,), EDGE_DEV // 2, EDGE_DEV + 1)
    busiest = jax.random.randint(pick_key, (), 0, SHARDS)
    return jnp.where(jnp.arange(SHARDS) == busiest, EDGE_DEV, counts).astype(jnp.int32)


def with_ends(result, rng, least, high):
    longest = result.shape.index(max(result.shape))
    spots = []
    for shift in (0, 1):
        where = [jax.random.randint(jax.random.fold_in(rng, axis), (), 0, length) for axis, length in enumerate(result.shape)]
        where[longest] = (where[longest] + shift) % result.shape[longest]
        spots.append(tuple(where))
    return result.at[spots[0]].set(least).at[spots[1]].set(high)


def shard_levels(own_key, dims, shards, least, high):
    def one(dim, parts):
        steps = jax.random.uniform(jax.random.fold_in(jax.random.fold_in(own_key, 6), dim), (parts,), jnp.float32, least / len(shards), high / len(shards))
        return jnp.repeat(jnp.exp(steps), dims[dim] // parts).reshape((-1,) + (1,) * (len(dims) - dim - 1))

    loudness = one(*shards[0])
    for cut in shards[1:]:
        loudness = loudness * one(*cut)
    return loudness


def gaussian(own_key, shape, deviation, most, pieces=(), kind=jnp.bfloat16):
    result = deviation * jax.random.normal(own_key, shape, jnp.float32)
    if pieces:
        result = result * shard_levels(own_key, shape, pieces, -0.22, 0.18)
    return jnp.clip(result, -most, most).astype(kind)


def setup_inputs(seed: int = 0) -> dict:
    seeds = jax.random.split(jax.random.key(seed), 20)
    nodes = gaussian(seeds[0], (NODES, D), 1.0, 6.0, ((0, 32), (1, 4)))
    edges = gaussian(seeds[1], (EDGES, D), 1.0, 6.0, ((0, 128),))
    senders = with_ends(jax.random.randint(seeds[2], (EDGES,), 0, TABLE), jax.random.fold_in(seeds[2], 1), 0, TABLE - 1).astype(jnp.int32)
    receivers = with_ends(jax.random.randint(seeds[3], (EDGES,), 0, NODE_DEV), jax.random.fold_in(seeds[3], 1), 0, NODE_DEV - 1).astype(jnp.int32)
    halo_rows = with_ends(jax.random.randint(seeds[4], (PATCHES, 2, HALO), 0, NODE_DEV), jax.random.fold_in(seeds[4], 1), 0, NODE_DEV - 1).astype(jnp.int32)
    coarse_rows = with_ends(jax.random.randint(seeds[5], (PATCHES, PATCHES, SLOT), 0, COARSE_DEV), jax.random.fold_in(seeds[5], 1), 0, COARSE_DEV - 1).astype(jnp.int32)
    edge_count = draw_edge_count(jax.random.fold_in(seeds[19], 71), 0)
    w_edge_in = gaussian(seeds[7], (3 * D, D), (3 * D) ** -0.5, 0.15625)
    b_edge_in = gaussian(seeds[8], (D,), 0.5, 3.0, (), jnp.float32)
    w_edge_out = gaussian(seeds[9], (D, D), D ** -0.5, 0.25)
    b_edge_out = gaussian(seeds[10], (D,), 0.3, 2.0, (), jnp.float32)
    edge_gain = jnp.clip(1.0 + 0.1 * jax.random.normal(seeds[11], (D,), jnp.float32), 0.5, 1.5)
    edge_shift = gaussian(seeds[12], (D,), 0.2, 1.0, (), jnp.float32)
    w_node_in = gaussian(seeds[13], (2 * D, D), (2 * D) ** -0.5, 0.1875)
    b_node_in = gaussian(seeds[14], (D,), 0.5, 3.0, (), jnp.float32)
    w_node_out = gaussian(seeds[15], (D, D), D ** -0.5, 0.25)
    b_node_out = gaussian(seeds[16], (D,), 0.3, 2.0, (), jnp.float32)
    node_gain = jnp.clip(1.0 + 0.1 * jax.random.normal(seeds[17], (D,), jnp.float32), 0.5, 1.5)
    node_shift = gaussian(seeds[18], (D,), 0.2, 1.0, (), jnp.float32)
    return {"nodes": nodes, "edges": edges, "senders": senders, "receivers": receivers, "halo_rows": halo_rows, "coarse_rows": coarse_rows, "edge_count": edge_count, "w_edge_in": w_edge_in, "b_edge_in": b_edge_in, "w_edge_out": w_edge_out, "b_edge_out": b_edge_out, "edge_gain": edge_gain, "edge_shift": edge_shift, "w_node_in": w_node_in, "b_node_in": b_node_in, "w_node_out": w_node_out, "b_node_out": b_node_out, "node_gain": node_gain, "node_shift": node_shift}


layer_epsilon = 1e-05

def perceptron(inputs, weight_in, bias_in, weight_out, bias_out, norm_gain, norm_shift):
    joined = jnp.concatenate(inputs, axis=1)
    hidden = jnp.dot(joined, weight_in, preferred_element_type=jnp.float32) + bias_in
    active = jax.nn.silu(hidden).astype(jnp.bfloat16)
    output = jnp.dot(active, weight_out, preferred_element_type=jnp.float32) + bias_out
    row_mean = lax.optimization_barrier(jnp.mean(output, axis=1, keepdims=True))
    row_var = lax.optimization_barrier(jnp.mean(jnp.square(output - row_mean), axis=1, keepdims=True))
    return (output - row_mean) * lax.rsqrt(row_var + layer_epsilon) * norm_gain + norm_shift

def block_segments(values, targets):
    return jax.ops.segment_sum(values, targets, num_segments=NODE_DEV)

def reference(nodes, edges, senders, receivers, halo_rows, coarse_rows, edge_count, w_edge_in, b_edge_in, w_edge_out, b_edge_out, edge_gain, edge_shift, w_node_in, b_node_in, w_node_out, b_node_out, node_gain, node_shift):
    patch_edges = N_HIDDEN * EDGE_DEV

    def patch_work(patch_id):
        first_edge = patch_id * patch_edges
        latent = lax.dynamic_slice_in_dim(edges, first_edge, patch_edges, 0)
        sender_code = lax.dynamic_slice_in_dim(senders, first_edge, patch_edges, 0)
        target = lax.dynamic_slice_in_dim(receivers, first_edge, patch_edges, 0)
        counts = lax.dynamic_slice_in_dim(edge_count, patch_id * N_HIDDEN, N_HIDDEN, 0)
        previous = jnp.mod(patch_id - 1, PATCHES).astype(jnp.int32)
        following = jnp.mod(patch_id + 1, PATCHES).astype(jnp.int32)
        from_previous = halo_rows[previous, 1][jnp.clip(sender_code - NODE_DEV, 0, HALO - 1)]
        from_following = halo_rows[following, 0][jnp.clip(sender_code - NODE_DEV - HALO, 0, HALO - 1)]
        far_slot = jnp.clip(sender_code - NODE_DEV - 2 * HALO, 0, PATCHES * SLOT - 1)
        far_owner = far_slot // SLOT
        far_row = coarse_rows[patch_id][far_owner, far_slot % SLOT]
        source = jnp.where(sender_code < NODE_DEV, patch_id * NODE_DEV + sender_code, jnp.where(sender_code < NODE_DEV + HALO, previous * NODE_DEV + from_previous, jnp.where(sender_code < NODE_DEV + 2 * HALO, following * NODE_DEV + from_following, far_owner * NODE_DEV + far_row))).astype(jnp.int32)
        sender_rows = nodes[source]
        patch_nodes = lax.dynamic_slice_in_dim(nodes, patch_id * NODE_DEV, NODE_DEV, 0)
        receiver_rows = patch_nodes[target]
        update = perceptron((latent, sender_rows, receiver_rows), w_edge_in, b_edge_in, w_edge_out, b_edge_out, edge_gain, edge_shift)
        position = jnp.arange(patch_edges, dtype=jnp.int32)
        live_mask = position % EDGE_DEV < counts[position // EDGE_DEV]
        message = jnp.where(live_mask[:, None], update, jnp.zeros_like(update))
        new_latent = (latent.astype(jnp.float32) + message).astype(jnp.bfloat16)
        sent = lax.optimization_barrier(message.astype(jnp.bfloat16)).astype(jnp.float32)
        partial_sums = jax.vmap(block_segments)(sent.reshape(N_HIDDEN, EDGE_DEV, D), target.reshape(N_HIDDEN, EDGE_DEV))
        rounded = lax.optimization_barrier(partial_sums.astype(jnp.bfloat16)).astype(jnp.float32)
        node_sums = lax.optimization_barrier(jnp.sum(rounded, axis=0))
        return (new_latent, node_sums)
    new_edges, node_sums = lax.map(patch_work, jnp.arange(PATCHES, dtype=jnp.int32))
    edges_out = new_edges.reshape(EDGES, D)
    gathered = node_sums.reshape(NODES, D).astype(jnp.bfloat16)
    update = perceptron((nodes, gathered), w_node_in, b_node_in, w_node_out, b_node_out, node_gain, node_shift)
    nodes_out = (nodes.astype(jnp.float32) + update).astype(jnp.bfloat16)
    return (nodes_out, edges_out)
```

```python
import functools

import jax
import jax.numpy as jnp
from jax import lax
from jax.experimental import pallas as pl
from jax.experimental.pallas import tpu as pltpu
from jax.sharding import PartitionSpec as P

COARSE_DEV = 64
layer_epsilon = 1e-05
BLK = 128
bf16 = jnp.bfloat16
f32 = jnp.float32
i32 = jnp.int32

VM = pl.BlockSpec(memory_space=pltpu.VMEM)
SM = pl.BlockSpec(memory_space=pltpu.SMEM)
ANY = pl.BlockSpec(memory_space=pl.ANY)
PARAMS = pltpu.CompilerParams(vmem_limit_bytes=56 * 1024 * 1024)


def dot(a, b):
    return jnp.dot(a, b, preferred_element_type=f32)


def cost(flops, nbytes):
    return pl.CostEstimate(flops=int(flops), bytes_accessed=int(nbytes), transcendentals=0)


def normalize(output, gain, shift):
    width = output.shape[1]
    mean = jnp.sum(output, axis=1, keepdims=True) * (1.0 / width)
    centered = output - mean
    var = jnp.sum(centered * centered, axis=1, keepdims=True) * (1.0 / width)
    return centered * lax.rsqrt(var + layer_epsilon) * gain + shift


def order_kernel(scal, recv, pos_out, meta_out):
    h = scal[0]
    live = scal[1]
    rows, lanes = recv.shape
    chunk_bits = (rows * lanes // 4).bit_length() - 1
    number = lax.broadcasted_iota(i32, (rows, lanes), 0) * lanes + lax.broadcasted_iota(
        i32, (rows, lanes), 1
    )
    rel = (lax.shift_right_logical(recv[...], chunk_bits) - h) & 3
    turn = jnp.where(rel == 2, 0, jnp.where(rel == 1, 1, jnp.where(rel == 3, 2, 3)))
    turn = jnp.where(number < live, turn, 4)
    upper = (
        lax.broadcasted_iota(i32, (lanes, lanes), 0) < lax.broadcasted_iota(i32, (lanes, lanes), 1)
    ).astype(f32)
    lower = (
        lax.broadcasted_iota(i32, (rows, rows), 1) < lax.broadcasted_iota(i32, (rows, rows), 0)
    ).astype(f32)
    start = jnp.zeros((1, 1), i32)
    pos = jnp.zeros((rows, lanes), i32)
    lane = lax.broadcasted_iota(i32, (8, 128), 1)
    row8 = lax.broadcasted_iota(i32, (8, 128), 0)
    meta = jnp.zeros((8, 128), i32)
    for v in range(5):
        hit = turn == v
        m = hit.astype(f32)
        within = dot(m, upper)
        above = jnp.sum(dot(lower, m), axis=1, keepdims=True)
        count = jnp.sum(jnp.sum(m, axis=1, keepdims=True), axis=0, keepdims=True).astype(i32)
        pos = jnp.where(hit, start + (within + above).astype(i32), pos)
        meta = jnp.where((row8 == 0) & (lane == v), start, meta)
        meta = jnp.where((row8 == 1) & (lane == v), count, meta)
        start = start + ((count + (BLK - 1)) & ~(BLK - 1))
    pos_out[...] = pos
    meta_out[...] = meta


def edge_term_kernel(pos, send, recv, edges, w, b, out, code_out, recv_out, tmp):
    slots = code_out.shape[0]

    def clear(i, c):
        for j in range(BLK):
            code_out[i * BLK + j] = 0
            recv_out[i * BLK + j] = -1
        return c

    lax.fori_loop(0, slots // BLK, clear, 0)

    def block(i, c):
        base = pl.multiple_of(i * BLK, BLK)
        x = dot(edges[pl.ds(base, BLK), :], w[...]) + b[...]
        for k in range(4):
            tmp[pl.ds(k, BLK, stride=4), :] = x[:, 128 * k : 128 * (k + 1)]
        for j in range(BLK):
            p = pos[base + j]
            out[pl.ds(pl.multiple_of(p * 4, 4), 4), :] = tmp[4 * j : 4 * j + 4, :]
            code_out[p] = send[base + j]
            recv_out[p] = recv[base + j]
        return c

    lax.fori_loop(0, edges.shape[0] // BLK, block, 0)


def project_kernel(halo, s0, s1a, s1b, s2a, s2b, s3a, s3b, w, x_out, p_out, back, forw, tmp):
    half = s1a.shape[0]
    n = 2 * half
    x_out[:, 0:128] = s0[...]
    for k, (a, b) in ((1, (s1a, s1b)), (2, (s2a, s2b)), (3, (s3a, s3b))):
        x_out[0:half, 128 * k : 128 * (k + 1)] = a[...]
        x_out[half:n, 128 * k : 128 * (k + 1)] = b[...]

    def proj(i, c):
        base = pl.multiple_of(i * 256, 256)
        y = dot(x_out[pl.ds(base, 256), :], w[...])
        for k in range(4):
            p_out[pl.ds(base * 4 + k, 256, stride=4), :] = y[:, 128 * k : 128 * (k + 1)]
        return c

    lax.fori_loop(0, n // 256, proj, 0)
    for side, dst in ((0, back), (1, forw)):

        def rows(i, c):
            base = pl.multiple_of(i * BLK, BLK)
            for j in range(BLK):
                r = halo[side * back.shape[0] + base + j]
                tmp[4 * j : 4 * j + 4, :] = p_out[pl.ds(pl.multiple_of(r * 4, 4), 4), :]
            for k in range(4):
                dst[pl.ds(base, BLK), 128 * k : 128 * (k + 1)] = tmp[
                    pl.ds(k, BLK, stride=4), :
                ].astype(bf16)
            return c

        lax.fori_loop(0, back.shape[0] // BLK, rows, 0)


def receiver_kernel(meta, scal, recv, x, w, term, out, tab):
    n = x.shape[0]
    quarter = n // 4
    h = scal[0]

    def proj(i, c):
        base = pl.multiple_of(i * 256, 256)
        tab[pl.ds(base, 256), :] = dot(x[pl.ds(base, 256), :], w[...]).astype(bf16)
        return c

    lax.fori_loop(0, n // 256, proj, 0)
    for v, rel in enumerate((2, 1, 3, 0)):
        chunk = (h + rel) & 3
        first = pl.multiple_of(chunk * quarter, quarter)
        start = meta[0, v]
        blocks = (meta[1, v] + (BLK - 1)) // BLK

        def block(i, c):
            s = pl.multiple_of(start + i * BLK, BLK)
            target = recv[pl.ds(s // BLK, 1), :] - first
            hot = (lax.broadcasted_iota(i32, (quarter, BLK), 0) == target).astype(bf16)
            got = lax.dot_general(
                hot,
                tab[pl.ds(first, quarter), :],
                (((0,), (0,)), ((), ())),
                preferred_element_type=f32,
            )
            for k in range(4):
                out[pl.ds(s, BLK), 128 * k : 128 * (k + 1)] = (
                    term[pl.ds(s * 4 + k, BLK, stride=4), :] + got[:, 128 * k : 128 * (k + 1)]
                )
            return c

        lax.fori_loop(0, blocks, block, 0)


def message_kernel(
    turns,
    meta,
    scal,
    code,
    recv,
    own,
    prev,
    nxt,
    c0,
    c1,
    c2,
    c3,
    w_send,
    term,
    w,
    b,
    gain,
    shift,
    *rest,
):
    rest = rest[-(2 * len(turns) + 6) :]
    outs = rest[: 2 * len(turns)]
    msg_out = rest[2 * len(turns)]
    tab, tmp, acc, buf, sem = rest[2 * len(turns) + 1 :]
    n4 = own.shape[0]
    border = prev.shape[0]
    quarter = n4 // 16
    h = scal[0]
    load = pltpu.make_async_copy(own, tab.at[pl.ds(0, n4), :], sem)
    load.start()
    for t, src in ((0, prev), (1, nxt)):

        def conv(i, c):
            base = pl.multiple_of(i * 256, 256)
            for k in range(4):
                tab[pl.ds(n4 + t * 4 * border + base * 4 + k, 256, stride=4), :] = src[
                    pl.ds(base, 256), 128 * k : 128 * (k + 1)
                ].astype(f32)
            return c

        lax.fori_loop(0, border // 256, conv, 0)
    far = c0.shape[0]
    y = dot(c0[...], w_send[0:128, :])
    y = y + dot(c1[...], w_send[128:256, :])
    y = y + dot(c2[...], w_send[256:384, :])
    y = y + dot(c3[...], w_send[384:512, :])
    for k in range(4):
        tab[pl.ds(n4 + 8 * border + k, far, stride=4), :] = y[:, 128 * k : 128 * (k + 1)]
    load.wait()
    for slot, v in enumerate(turns):
        rel = (2, 1, 3, 0)[v]
        first = ((h + rel) & 3) * quarter
        start = meta[0, v]
        count = meta[1, v]
        blocks = (count + (BLK - 1)) // BLK
        acc[...] = jnp.zeros_like(acc)

        def block(i, c):
            s = pl.multiple_of(start + i * BLK, BLK)
            for j in range(BLK):
                r = code[s + j]
                tmp[4 * j : 4 * j + 4, :] = tab[pl.ds(pl.multiple_of(r * 4, 4), 4), :]
            parts = []
            for k in range(4):
                pre = (
                    term[pl.ds(s, BLK), 128 * k : 128 * (k + 1)] + tmp[pl.ds(k, BLK, stride=4), :]
                )
                parts.append((pre / (1.0 + jnp.exp(-pre))).astype(bf16))
            active = jnp.concatenate(parts, axis=1)
            update = normalize(dot(active, w[...]) + b[...], gain[...], shift[...])
            valid = lax.broadcasted_iota(i32, (BLK, 1), 0) + i * BLK < count
            message = jnp.where(valid, update, 0.0)
            for k in range(4):
                buf[pl.ds(k, BLK, stride=4), :] = message[:, 128 * k : 128 * (k + 1)]
            target = recv[pl.ds(s // BLK, 1), :] - first
            hot = (lax.broadcasted_iota(i32, (quarter, BLK), 0) == target).astype(bf16)
            acc[...] += dot(hot, message.astype(bf16))
            save = pltpu.make_async_copy(
                buf, msg_out.at[pl.ds(pl.multiple_of(s * 4, 4 * BLK), 4 * BLK), :], sem
            )
            save.start()
            save.wait()
            return c

        lax.fori_loop(0, blocks, block, 0)
        outs[2 * slot][...] = acc[0 : quarter // 2, :].astype(bf16)
        outs[2 * slot + 1][...] = acc[quarter // 2 : quarter, :].astype(bf16)


def edges_out_kernel(scal, pos, edges, msg, out, tmp):
    live = scal[1]

    def block(i, c):
        base = pl.multiple_of(i * BLK, BLK)
        for j in range(BLK):
            p = pos[base + j]
            tmp[4 * j : 4 * j + 4, :] = msg[pl.ds(pl.multiple_of(p * 4, 4), 4), :]
        valid = lax.broadcasted_iota(i32, (BLK, 1), 0) + base < live
        for k in range(4):
            old = edges[pl.ds(base, BLK), 128 * k : 128 * (k + 1)].astype(f32)
            add = jnp.where(valid, tmp[pl.ds(k, BLK, stride=4), :], 0.0)
            out[pl.ds(base, BLK), 128 * k : 128 * (k + 1)] = (old + add).astype(bf16)
        return c

    lax.fori_loop(0, edges.shape[0] // BLK, block, 0)


def node_kernel(
    rows, ownA, ownB, upA, upB, downA, downB, w1, w2, b1, w3, b3, gain, shift, o0, o1, o2, o3
):
    half = ownA.shape[0]
    for t, (own, up, down) in enumerate(((ownA, upA, downA), (ownB, upB, downB))):
        total = own[...].astype(f32) + up[...].astype(f32) + down[...].astype(f32)
        x = rows[t * half : (t + 1) * half, :]
        pre = dot(x, w1[...]) + dot(total.astype(bf16), w2[...]) + b1[...]
        active = (pre / (1.0 + jnp.exp(-pre))).astype(bf16)
        update = normalize(dot(active, w3[...]) + b3[...], gain[...], shift[...])
        new = (x.astype(f32) + update).astype(bf16)
        for k, o in enumerate((o0, o1, o2, o3)):
            o[t * half : (t + 1) * half, :] = new[:, 128 * k : 128 * (k + 1)]


def sds(shape, dtype):
    return jax.ShapeDtypeStruct(shape, dtype)


def shifted(array, step):
    n = lax.axis_size("hidden")
    return lax.ppermute(array, "hidden", [(i, (i + step) % n) for i in range(n)])


def chained(array, step):
    n = lax.axis_size("patch")
    return lax.ppermute(array, "patch", [(i, (i + step) % n) for i in range(n)])


def rolled(array, h, axis):
    width = array.shape[axis]
    twice = jnp.concatenate([array, array], axis=axis)
    return lax.dynamic_slice_in_dim(twice, h * (width // 4), width, axis)


def local(
    nodes,
    edges,
    senders,
    receivers,
    halo_rows,
    coarse_rows,
    edge_count,
    w_edge_in,
    b_edge_in,
    w_edge_out,
    b_edge_out,
    edge_gain,
    edge_shift,
    w_node_in,
    b_node_in,
    w_node_out,
    b_node_out,
    node_gain,
    node_shift,
):
    n = nodes.shape[0]
    d = edges.shape[1]
    ne = edges.shape[0]
    half = n // 2
    quarter = n // 4
    border = halo_rows.shape[2]
    patches = lax.axis_size("patch")
    slots = ne + 4 * BLK
    h = lax.axis_index("hidden")
    scal = jnp.stack([h, edge_count[0]]).astype(i32)

    top = nodes[:half]
    bottom = nodes[half:]
    upA = shifted(top, 1)
    dnB = shifted(bottom, -1)
    upB = shifted(bottom, 1)
    dnA = shifted(top, -1)
    farA = shifted(upA, 1)
    farB = shifted(dnB, -1)

    mine = jnp.broadcast_to(nodes[None, :COARSE_DEV], (patches, COARSE_DEV, nodes.shape[1]))
    everyone = lax.all_to_all(mine, "patch", 0, 0, tiled=True).reshape(patches * COARSE_DEV, -1)
    owner_start = jnp.arange(patches, dtype=i32)[:, None] * COARSE_DEV
    c0 = everyone[(owner_start + coarse_rows[0]).reshape(-1)]
    c3 = shifted(c0, 1)
    c1 = shifted(c0, -1)
    c2 = shifted(c0, 2)

    row = lambda v: v.reshape(1, -1)
    w_self = w_edge_in[:d]
    w_send = rolled(w_edge_in[d : 2 * d], h, 0)
    w_recv = rolled(w_edge_in[2 * d :], h, 0)

    pos, meta = pl.pallas_call(
        order_kernel,
        out_shape=(sds((ne // 128, 128), i32), sds((8, 128), i32)),
        in_specs=[SM, VM],
        out_specs=(VM, VM),
        name="order",
        cost_estimate=cost(1e6, 1e5),
    )(scal, receivers.reshape(ne // 128, 128))
    pos = pos.reshape(ne)
    term, code, recv = pl.pallas_call(
        edge_term_kernel,
        out_shape=(sds((slots * 4, 128), f32), sds((slots,), i32), sds((slots,), i32)),
        in_specs=[SM, SM, SM, VM, VM, VM],
        out_specs=(VM, SM, SM),
        scratch_shapes=[pltpu.VMEM((4 * BLK, 128), f32)],
        compiler_params=PARAMS,
        name="edge_term",
        cost_estimate=cost(8e9, 8e6),
    )(pos, senders, receivers, edges, w_self, row(b_edge_in))
    recv2 = recv.reshape(slots // BLK, BLK)

    x, own, back, forw = pl.pallas_call(
        project_kernel,
        out_shape=(
            sds((n, d), bf16),
            sds((n * 4, 128), f32),
            sds((border, d), bf16),
            sds((border, d), bf16),
        ),
        in_specs=[SM] + [VM] * 8,
        out_specs=(VM, VM, VM, VM),
        scratch_shapes=[pltpu.VMEM((4 * BLK, 128), f32)],
        compiler_params=PARAMS,
        name="project",
        cost_estimate=cost(4e9, 1e7),
    )(halo_rows.reshape(-1), nodes, dnA, dnB, farA, farB, upA, upB, w_send)
    prev = chained(forw, 1)
    nxt = chained(back, -1)

    term2 = pl.pallas_call(
        receiver_kernel,
        out_shape=sds((slots, d), f32),
        in_specs=[SM, SM] + [VM] * 4,
        out_specs=VM,
        scratch_shapes=[pltpu.VMEM((n, d), bf16)],
        compiler_params=PARAMS,
        name="receiver",
        cost_estimate=cost(4e9, 1e7),
    )(meta, scal, recv2, x, w_recv, term)

    def messages(turns, msg):
        outs = []
        for _ in turns:
            outs += [sds((quarter // 2, d), bf16)] * 2
        res = pl.pallas_call(
            functools.partial(message_kernel, turns),
            out_shape=tuple(outs) + (sds((slots * 4, 128), f32),),
            in_specs=[SM, SM, SM] + [VM, ANY] + [VM] * 12 + [ANY] * len(msg),
            out_specs=tuple([VM] * len(outs)) + (ANY,),
            scratch_shapes=[
                pltpu.VMEM((4 * (n + 2 * border + c0.shape[0]), 128), f32),
                pltpu.VMEM((4 * BLK, 128), f32),
                pltpu.VMEM((quarter, d), f32),
                pltpu.VMEM((4 * BLK, 128), f32),
                pltpu.SemaphoreType.DMA,
            ],
            input_output_aliases={17: len(outs)} if msg else {},
            compiler_params=PARAMS,
            name="messages" + str(turns[0]),
            cost_estimate=cost(3e9 * len(turns), 1e7),
        )(
            meta,
            scal,
            code,
            recv2,
            own,
            prev,
            nxt,
            c0,
            c1,
            c2,
            c3,
            w_send,
            term2,
            w_edge_out,
            row(b_edge_out),
            row(edge_gain),
            row(edge_shift),
            *msg,
        )
        return res[:-1], res[-1]

    (a0, b0), msg = messages((0,), ())
    gotA = shifted(a0, 1)
    gotB = shifted(b0, -1)
    (a1, b1, a2, b2), msg = messages((1, 2), (msg,))
    upB = shifted(b1, 1)
    downA = shifted(a2, -1)
    (a3, b3), msg = messages((3,), (msg,))
    a1 = (a1.astype(f32) + gotA.astype(f32)).astype(bf16)
    b2 = (b2.astype(f32) + gotB.astype(f32)).astype(bf16)
    upA = shifted(a1, 1)
    downB = shifted(b2, -1)

    edges_out = pl.pallas_call(
        edges_out_kernel,
        out_shape=sds((ne, d), bf16),
        in_specs=[SM, SM, VM, VM],
        out_specs=VM,
        scratch_shapes=[pltpu.VMEM((4 * BLK, 128), f32)],
        compiler_params=PARAMS,
        name="edges_out",
        cost_estimate=cost(4e9, 1e7),
    )(scal, pos, edges, msg)

    rows = lax.dynamic_slice_in_dim(x, h * quarter, quarter, 0)
    o0, o1, o2, o3 = pl.pallas_call(
        node_kernel,
        out_shape=tuple([sds((quarter, 128), bf16)] * 4),
        in_specs=[VM] * 14,
        out_specs=tuple([VM] * 4),
        compiler_params=PARAMS,
        name="node",
        cost_estimate=cost(2e9, 4e6),
    )(
        rows,
        a3,
        b3,
        upA,
        upB,
        downA,
        downB,
        rolled(w_node_in[:d], h, 0),
        w_node_in[d:],
        row(b_node_in),
        rolled(w_node_out, h, 1),
        row(rolled(b_node_out, h, 0)),
        row(rolled(node_gain, h, 0)),
        row(rolled(node_shift, h, 0)),
    )
    from_prev = shifted(o1, 1)
    from_next = shifted(o3, -1)
    from_far = shifted(o2, 2)
    result = jnp.concatenate([o0, from_next, from_far, from_prev], axis=0)
    twice = jnp.concatenate([result, result], axis=0)
    nodes_out = lax.dynamic_slice_in_dim(twice, ((4 - h) % 4) * quarter, n, 0)
    return (nodes_out, edges_out)


def solution(mesh):
    return jax.shard_map(
        local,
        mesh=mesh,
        in_specs=(
            P("patch", "hidden"),
            P(("patch", "hidden"), None),
            P(("patch", "hidden")),
            P(("patch", "hidden")),
            P("patch", None, None),
            P("patch", None, None),
            P(("patch", "hidden")),
        )
        + (P(),) * 12,
        out_specs=(P("patch", "hidden"), P(("patch", "hidden"), None)),
        check_vma=False,
    )
```

```python
import functools

import jax
import jax.numpy as jnp
from jax import lax
from jax.experimental import pallas as pl
from jax.experimental.pallas import tpu as pltpu
from jax.sharding import PartitionSpec as P

COARSE_DEV = 64
SLOT = 8
layer_epsilon = 1e-05
BLK = 128
BIG = 256
GRP = 16
WORD_BITS = 13
WORD = 1 << WORD_BITS
bf16 = jnp.bfloat16
f32 = jnp.float32
i32 = jnp.int32

VM = pl.BlockSpec(memory_space=pltpu.VMEM)
SM = pl.BlockSpec(memory_space=pltpu.SMEM)
ANY = pl.BlockSpec(memory_space=pl.ANY)
PARAMS = pltpu.CompilerParams(vmem_limit_bytes=12 * 1024 * 1024)


def dot(a, b):
    return jnp.dot(a, b, preferred_element_type=f32)


def cost(flops, nbytes):
    return pl.CostEstimate(flops=int(flops), bytes_accessed=int(nbytes), transcendentals=0)


def normalize(output, gain, shift):
    width = output.shape[1]
    mean = jnp.sum(output, axis=1, keepdims=True) * (1.0 / width)
    centered = output - mean
    var = jnp.sum(centered * centered, axis=1, keepdims=True) * (1.0 / width)
    return centered * lax.rsqrt(var + layer_epsilon) * gain + shift


def order_kernel(live_ref, send, recv, coarse, coarse_out, pos_out, word_out, meta_out):
    h = lax.axis_index("hidden")
    live = live_ref[0]
    rows, lanes = recv.shape
    chunk_bits = (rows * lanes // 4).bit_length() - 1
    number = lax.broadcasted_iota(i32, (rows, lanes), 0) * lanes + lax.broadcasted_iota(
        i32, (rows, lanes), 1
    )
    rel = (lax.shift_right_logical(recv[...], chunk_bits) - h) & 3
    turn = jnp.where(rel == 2, 0, jnp.where(rel == 1, 1, jnp.where(rel == 3, 2, 3)))
    turn = jnp.where(number < live, turn, 4)
    upper = (
        lax.broadcasted_iota(i32, (lanes, lanes), 0) < lax.broadcasted_iota(i32, (lanes, lanes), 1)
    ).astype(f32)
    lower = (
        lax.broadcasted_iota(i32, (rows, rows), 1) < lax.broadcasted_iota(i32, (rows, rows), 0)
    ).astype(f32)
    start = jnp.zeros((1, 1), i32)
    pos = jnp.zeros((rows, lanes), i32)
    lane = lax.broadcasted_iota(i32, (8, 128), 1)
    row8 = lax.broadcasted_iota(i32, (8, 128), 0)
    meta = jnp.zeros((8, 128), i32)
    for v in range(5):
        hit = turn == v
        m = hit.astype(f32)
        within = dot(m, upper)
        above = jnp.sum(dot(lower, m), axis=1, keepdims=True)
        count = jnp.sum(jnp.sum(m, axis=1, keepdims=True), axis=0, keepdims=True).astype(i32)
        pos = jnp.where(hit, start + (within + above).astype(i32), pos)
        meta = jnp.where((row8 == 0) & (lane == v), start, meta)
        meta = jnp.where((row8 == 1) & (lane == v), count, meta)
        start = start + ((count + (BLK - 1)) & ~(BLK - 1))
    far = coarse.shape[1]
    owner = lax.broadcasted_iota(i32, (1, far), 1) // SLOT
    coarse_out[...] = coarse[...] + owner * COARSE_DEV
    pos_out[...] = pos
    word_out[...] = send[...] + recv[...] * WORD
    meta_out[...] = meta


def edge_term_kernel(pos, word, meta, edges, w, b, out, word_out, tmp):
    d = w.shape[1]
    for v in range(4):
        last = meta[0, v + 1] - BLK

        @pl.when(meta[1, v] > 0)
        def _():
            for j in range(BLK):
                word_out[last + j] = 0

    def block(i, c):
        base = pl.multiple_of(i * BIG, BIG)
        x = dot(edges[pl.ds(base, BIG), :], w[0:d, :]) + b[...]
        for k in range(4):
            tmp[pl.ds(k, BIG, stride=4), :] = x[:, 128 * k : 128 * (k + 1)]
        for g in range(0, BIG, GRP):
            slots = [pos[base + g + j] for j in range(GRP)]
            words = [word[base + g + j] for j in range(GRP)]
            for j in range(GRP):
                word_out[slots[j]] = words[j]
            for j in range(GRP):
                out[pl.ds(pl.multiple_of(slots[j] * 4, 4), 4), :] = tmp[
                    4 * (g + j) : 4 * (g + j) + 4, :
                ]
        return c

    lax.fori_loop(0, edges.shape[0] // BIG, block, 0)


def roll_rows(dst, w, offset, h):
    for k in range(4):
        first = pl.multiple_of(offset + 128 * ((h + k) & 3), 128)
        dst[128 * k : 128 * (k + 1), :] = w[pl.ds(first, 128), :]


def project_kernel(halo, s0, s1, s2a, s2b, s3, w, after, x_out, tab, back, forw, tmp, wr):
    n = s0.shape[0]
    half = n // 2
    d = w.shape[1]
    roll_rows(wr, w, d, lax.axis_index("hidden"))
    x_out[:, 0:128] = s0[...]
    x_out[:, 128:256] = s1[...]
    x_out[0:half, 256:384] = s2a[...]
    x_out[half:n, 256:384] = s2b[...]
    x_out[:, 384:512] = s3[...]

    def proj(i, c):
        base = pl.multiple_of(i * 512, 512)
        y = dot(x_out[pl.ds(base, 512), :], wr[...])
        for k in range(4):
            tab[pl.ds(base * 4 + k, 512, stride=4), :] = y[:, 128 * k : 128 * (k + 1)]
        return c

    lax.fori_loop(0, n // 512, proj, 0)
    for side, dst in ((0, back), (1, forw)):

        def rows(i, c):
            base = pl.multiple_of(i * BIG, BIG)
            for j in range(BIG):
                r = halo[0, side, base + j]
                tmp[4 * j : 4 * j + 4, :] = tab[pl.ds(pl.multiple_of(r * 4, 4), 4), :]
            for k in range(4):
                dst[pl.ds(base, BIG), 128 * k : 128 * (k + 1)] = tmp[
                    pl.ds(k, BIG, stride=4), :
                ].astype(bf16)
            return c

        lax.fori_loop(0, back.shape[0] // BIG, rows, 0)


def over_blocks(count, big, small):
    rest = count & (BIG - 1)
    many = (count // BIG) + (rest > BLK).astype(i32)
    lax.fori_loop(0, many, big, 0)

    @pl.when((rest > 0) & (rest <= BLK))
    def _():
        small(many, 0)


def targets(word, s, size):
    row = s // BLK
    if size == BLK:
        both = word[pl.ds(row, 1), :]
    else:
        both = jnp.concatenate([word[pl.ds(row, 1), :], word[pl.ds(row + 1, 1), :]], axis=1)
    return lax.shift_right_logical(both, WORD_BITS)


def receiver_kernel(meta, word, x, w, term, out, tab, wr):
    n = x.shape[0]
    d = w.shape[1]
    quarter = n // 4
    h = lax.axis_index("hidden")
    roll_rows(wr, w, 2 * d, h)

    def proj(i, c):
        base = pl.multiple_of(i * 512, 512)
        tab[pl.ds(base, 512), :] = dot(x[pl.ds(base, 512), :], wr[...]).astype(bf16)
        return c

    lax.fori_loop(0, n // 512, proj, 0)
    for v, rel in enumerate((2, 1, 3, 0)):
        first = pl.multiple_of(((h + rel) & 3) * quarter, quarter)
        start = meta[0, v]

        def block(size, i, c):
            s = pl.multiple_of(start + i * BIG, BLK)
            target = targets(word, s, size) - first
            hot = (lax.broadcasted_iota(i32, (quarter, size), 0) == target).astype(bf16)
            got = lax.dot_general(
                hot,
                tab[pl.ds(first, quarter), :],
                (((0,), (0,)), ((), ())),
                preferred_element_type=f32,
            )
            for k in range(4):
                out[pl.ds(s, size), 128 * k : 128 * (k + 1)] = (
                    term[pl.ds(s * 4 + k, size, stride=4), :] + got[:, 128 * k : 128 * (k + 1)]
                )
            return c

        over_blocks(meta[1, v], functools.partial(block, BIG), functools.partial(block, BLK))


def chunk_messages(v, meta, h, word, words, tab, term, w, b, gain, shift, msg, tmp, acc):
    quarter = acc.shape[0]
    rel = (2, 1, 3, 0)[v]
    first = ((h + rel) & 3) * quarter
    start = meta[0, v]
    count = meta[1, v]
    acc[...] = jnp.zeros_like(acc)

    def block(size, i, c):
        s = pl.multiple_of(start + i * BIG, BLK)
        for j in range(size):
            r = word[s + j] & (WORD - 1)
            tmp[4 * j : 4 * j + 4, :] = tab[pl.ds(pl.multiple_of(r * 4, 4), 4), :]
        parts = []
        for k in range(4):
            pre = term[pl.ds(s, size), 128 * k : 128 * (k + 1)] + tmp[pl.ds(k, size, stride=4), :]
            parts.append((pre / (1.0 + jnp.exp(-pre))).astype(bf16))
        active = jnp.concatenate(parts, axis=1)
        update = normalize(dot(active, w[...]) + b[...], gain[...], shift[...])
        valid = lax.broadcasted_iota(i32, (size, 1), 0) + i * BIG < count
        message = jnp.where(valid, update, 0.0)
        for k in range(4):
            msg[pl.ds(s * 4 + k, size, stride=4), :] = message[:, 128 * k : 128 * (k + 1)]
        target = targets(words, s, size) - first
        hot = (lax.broadcasted_iota(i32, (quarter, size), 0) == target).astype(bf16)
        acc[...] += dot(hot, message.astype(bf16))
        return c

    over_blocks(count, functools.partial(block, BIG), functools.partial(block, BLK))


def first_kernel(
    meta, word, words, prev, nxt, c0, c1, c2, c3, w_in, term, w, b, gain, shift, tab_in,
    top, bottom, msg, tab, tmp, acc,
):
    d = w.shape[1]
    border = prev.shape[0]
    far = c0.shape[0]
    n4 = tab.shape[0] - 8 * border - 4 * far
    h = lax.axis_index("hidden")
    for t, src in ((0, prev), (1, nxt)):

        def conv(i, c):
            base = pl.multiple_of(i * 256, 256)
            for k in range(4):
                tab[pl.ds(n4 + t * 4 * border + base * 4 + k, 256, stride=4), :] = src[
                    pl.ds(base, 256), 128 * k : 128 * (k + 1)
                ].astype(f32)
            return c

        lax.fori_loop(0, border // 256, conv, 0)
    y = jnp.zeros((far, d), f32)
    for k, c in enumerate((c0, c1, c2, c3)):
        y = y + dot(c[...], w_in[pl.ds(pl.multiple_of(d + 128 * ((h + k) & 3), 128), 128), :])
    for k in range(4):
        tab[pl.ds(n4 + 8 * border + k, far, stride=4), :] = y[:, 128 * k : 128 * (k + 1)]
    chunk_messages(0, meta, h, word, words, tab, term, w, b, gain, shift, msg, tmp, acc)
    half = acc.shape[0] // 2
    top[...] = acc[0:half, :].astype(bf16)
    bottom[...] = acc[half:, :].astype(bf16)


def own_kernel(
    meta, word, words, tab, term, w, b, gain, shift, msg_in, sums, msg, tmp, acc
):
    chunk_messages(3, meta, lax.axis_index("hidden"), word, words, tab, term, w, b, gain, shift, msg, tmp, acc)
    sums[...] = acc[...].astype(bf16)


def near_kernel(
    meta, word, words, tab, term, w, b, gain, shift, topgot, bottomgot, msg_in,
    up, down, msg, tmp, acc,
):
    half = acc.shape[0] // 2
    h = lax.axis_index("hidden")
    chunk_messages(1, meta, h, word, words, tab, term, w, b, gain, shift, msg, tmp, acc)
    up[0:half, :] = (acc[0:half, :] + topgot[...].astype(f32)).astype(bf16)
    up[half:, :] = acc[half:, :].astype(bf16)
    chunk_messages(2, meta, h, word, words, tab, term, w, b, gain, shift, msg, tmp, acc)
    down[0:half, :] = acc[0:half, :].astype(bf16)
    down[half:, :] = (acc[half:, :] + bottomgot[...].astype(f32)).astype(bf16)


def edges_out_kernel(live_ref, pos, edges, msg, out, tmp):
    live = live_ref[0]

    def block(i, c):
        base = pl.multiple_of(i * BIG, BIG)
        for j in range(BIG):
            p = pos[base + j]
            tmp[4 * j : 4 * j + 4, :] = msg[pl.ds(pl.multiple_of(p * 4, 4), 4), :]
        valid = lax.broadcasted_iota(i32, (BIG, 1), 0) + base < live
        for k in range(4):
            old = edges[pl.ds(base, BIG), 128 * k : 128 * (k + 1)].astype(f32)
            add = jnp.where(valid, tmp[pl.ds(k, BIG, stride=4), :], 0.0)
            out[pl.ds(base, BIG), 128 * k : 128 * (k + 1)] = (old + add).astype(bf16)
        return c

    lax.fori_loop(0, edges.shape[0] // BIG, block, 0)


def node_kernel(
    x, own, up, down, w1, b1, w2, b2, gain, shift, after, o0, o1, o2, o3, wr, wc, vec
):
    h = lax.axis_index("hidden")
    d = w2.shape[1]
    quarter = own.shape[0]
    roll_rows(wr, w1, 0, h)
    for k in range(4):
        cols = pl.ds(pl.multiple_of(128 * ((h + k) & 3), 128), 128)
        here = slice(128 * k, 128 * (k + 1))
        wc[:, here] = w2[:, cols]
        vec[0:1, here] = b2[:, cols]
        vec[1:2, here] = gain[:, cols]
        vec[2:3, here] = shift[:, cols]
    half = quarter // 2
    for t in range(2):
        rows = pl.ds(pl.multiple_of(h * quarter + t * half, half), half)
        part = slice(t * half, (t + 1) * half)
        total = own[part, :].astype(f32) + up[part, :].astype(f32) + down[part, :].astype(f32)
        mine = x[rows, :]
        pre = dot(mine, wr[...]) + dot(total.astype(bf16), w1[d : 2 * d, :]) + b1[...]
        active = (pre / (1.0 + jnp.exp(-pre))).astype(bf16)
        update = normalize(dot(active, wc[...]) + vec[0:1, :], vec[1:2, :], vec[2:3, :])
        new = (mine.astype(f32) + update).astype(bf16)
        for k, o in enumerate((o0, o1, o2, o3)):
            o[part, :] = new[:, 128 * k : 128 * (k + 1)]


def far_rows_kernel(index, everyone, out):
    far = out.shape[0]
    rows = everyone.shape[0]
    hot = lax.broadcasted_iota(i32, (rows, far), 0) == index[...]
    got = lax.dot_general(
        hot.astype(bf16),
        everyone[...],
        (((0,), (0,)), ((), ())),
        preferred_element_type=f32,
    )
    out[...] = got.astype(bf16)


def gather_out_kernel(p0, p1, p2, p3, out):
    quarter = p0.shape[0]
    h = lax.axis_index("hidden")
    for k, p in enumerate((p0, p1, p2, p3)):
        first = pl.multiple_of(((h + k) & 3) * quarter, quarter)
        out[pl.ds(first, quarter), :] = p[...]


def sds(shape, dtype):
    return jax.ShapeDtypeStruct(shape, dtype)


def shifted(array, step):
    n = lax.axis_size("hidden")
    return lax.ppermute(array, "hidden", [(i, (i + step) % n) for i in range(n)])


def chained(array, step):
    n = lax.axis_size("patch")
    return lax.ppermute(array, "patch", [(i, (i + step) % n) for i in range(n)])


def call(kernel, name, out_shape, in_specs, out_specs, scratch=(), flops=1e9, **kw):
    return pl.pallas_call(
        kernel,
        out_shape=out_shape,
        in_specs=in_specs,
        out_specs=out_specs,
        scratch_shapes=list(scratch),
        compiler_params=PARAMS,
        name=name,
        cost_estimate=cost(flops, 4e6),
        **kw,
    )


def local(
    nodes,
    edges,
    senders,
    receivers,
    halo_rows,
    coarse_rows,
    edge_count,
    w_edge_in,
    b_edge_in,
    w_edge_out,
    b_edge_out,
    edge_gain,
    edge_shift,
    w_node_in,
    b_node_in,
    w_node_out,
    b_node_out,
    node_gain,
    node_shift,
):
    n = nodes.shape[0]
    d = edges.shape[1]
    ne = edges.shape[0]
    half = n // 2
    quarter = n // 4
    border = halo_rows.shape[2]
    patches = lax.axis_size("patch")
    slots = ne + 4 * BLK

    up = shifted(nodes, 1)
    down = shifted(nodes, -1)
    farA = shifted(up[:half], 1)
    farB = shifted(down[half:], -1)

    mine = jnp.broadcast_to(nodes[None, :COARSE_DEV], (patches, COARSE_DEV, nodes.shape[1]))
    everyone = lax.all_to_all(mine, "patch", 0, 0, tiled=True).reshape(patches * COARSE_DEV, -1)
    far = coarse_rows.shape[1] * coarse_rows.shape[2]

    row = lambda v: v.reshape(1, -1)
    square = lambda v: v.reshape(ne // 128, 128)
    table = sds((4 * (n + 2 * border + far), 128), f32)
    spread = sds((slots * 4, 128), f32)
    rows_f32 = pltpu.VMEM((4 * BIG, 128), f32)
    weight = pltpu.VMEM((d, d), bf16)
    sums_acc = pltpu.VMEM((quarter, d), f32)

    index, pos, word, meta = call(
        order_kernel,
        "order",
        (
            sds((1, far), i32),
            sds((ne // 128, 128), i32),
            sds((ne // 128, 128), i32),
            sds((8, 128), i32),
        ),
        [SM, VM, VM, VM],
        (VM, VM, VM, VM),
    )(edge_count, square(senders), square(receivers), coarse_rows.reshape(1, far))
    c0 = call(far_rows_kernel, "far_rows", sds((far, nodes.shape[1]), bf16), [VM, VM], VM)(
        index, everyone
    )
    c3 = shifted(c0, 1)
    c1 = shifted(c0, -1)
    c2 = shifted(c0, 2)
    pos = pos.reshape(ne)
    term, word = call(
        edge_term_kernel,
        "edge_term",
        (spread, sds((slots,), i32)),
        [SM, SM, SM, VM, VM, VM],
        (VM, SM),
        [rows_f32],
        flops=6e9,
    )(pos, word.reshape(ne), meta, edges, w_edge_in, row(b_edge_in))
    words = word.reshape(slots // BLK, BLK)

    x, tab, back, forw = call(
        project_kernel,
        "project",
        (sds((n, d), bf16), table, sds((border, d), bf16), sds((border, d), bf16)),
        [SM] + [VM] * 6 + [ANY],
        (VM, VM, VM, VM),
        [rows_f32, weight],
        flops=6e9,
    )(halo_rows, nodes, down, farA, farB, up, w_edge_in, word)
    prev = chained(forw, 1)
    nxt = chained(back, -1)

    term = call(
        receiver_kernel,
        "receiver",
        sds((slots, d), f32),
        [SM] + [VM] * 4,
        VM,
        [pltpu.VMEM((n, d), bf16), weight],
        flops=5e9,
    )(meta, words, x, w_edge_in, term)

    layer = (w_edge_out, row(b_edge_out), row(edge_gain), row(edge_shift))
    part = sds((quarter // 2, d), bf16)
    whole = sds((quarter, d), bf16)
    top, bottom, msg, tab = call(
        first_kernel,
        "first",
        (part, part, spread, table),
        [SM, SM] + [VM] * 14,
        (VM, VM, VM, VM),
        [rows_f32, sums_acc],
        flops=3e9,
        input_output_aliases={15: 3},
    )(meta, word, words, prev, nxt, c0, c1, c2, c3, w_edge_in, term, *layer, tab)
    topgot = shifted(top, 1)
    bottomgot = shifted(bottom, -1)
    own, msg = call(
        own_kernel,
        "own",
        (whole, spread),
        [SM, SM] + [VM] * 8,
        (VM, VM),
        [rows_f32, sums_acc],
        flops=3e9,
        input_output_aliases={9: 1},
    )(meta, word, words, tab, term, *layer, msg)
    upsum, downsum, msg = call(
        near_kernel,
        "near",
        (whole, whole, spread),
        [SM, SM] + [VM] * 10,
        (VM, VM, VM),
        [rows_f32, sums_acc],
        flops=5e9,
        input_output_aliases={11: 2},
    )(meta, word, words, tab, term, *layer, topgot, bottomgot, msg)
    upsum = shifted(upsum, 1)
    downsum = shifted(downsum, -1)

    edges_out = call(
        edges_out_kernel,
        "edges_out",
        sds((ne, d), bf16),
        [SM, SM, VM, VM],
        VM,
        [rows_f32],
        flops=5e9,
    )(edge_count, pos, edges, msg)

    share = sds((quarter, 128), bf16)
    o0, o1, o2, o3 = call(
        node_kernel,
        "node",
        (share,) * 4,
        [VM] * 10 + [ANY],
        (VM,) * 4,
        [weight, weight, pltpu.VMEM((8, d), f32)],
    )(
        x,
        own,
        upsum,
        downsum,
        w_node_in,
        row(b_node_in),
        w_node_out,
        row(b_node_out),
        row(node_gain),
        row(node_shift),
        edges_out,
    )
    from_prev = shifted(o1, 1)
    from_next = shifted(o3, -1)
    from_far = shifted(o2, 2)
    nodes_out = call(
        gather_out_kernel, "gather_out", sds((n, 128), bf16), [VM] * 4, VM
    )(o0, from_next, from_far, from_prev)
    return (nodes_out, edges_out)


def solution(mesh):
    return jax.shard_map(
        local,
        mesh=mesh,
        in_specs=(
            P("patch", "hidden"),
            P(("patch", "hidden"), None),
            P(("patch", "hidden")),
            P(("patch", "hidden")),
            P("patch", None, None),
            P("patch", None, None),
            P(("patch", "hidden")),
        )
        + (P(),) * 12,
        out_specs=(P("patch", "hidden"), P(("patch", "hidden"), None)),
        check_vma=False,
    )
```

```python
import functools

import jax
import jax.numpy as jnp
from jax import lax
from jax.experimental import pallas as pl
from jax.experimental.pallas import tpu as pltpu
from jax.sharding import PartitionSpec as P

COARSE_DEV = 64
SLOT = 8
layer_epsilon = 1e-05
BLK = 128
BIG = 256
bf16 = jnp.bfloat16
f32 = jnp.float32
i32 = jnp.int32

VM = pl.BlockSpec(memory_space=pltpu.VMEM)
SM = pl.BlockSpec(memory_space=pltpu.SMEM)
ANY = pl.BlockSpec(memory_space=pl.ANY)
PARAMS = pltpu.CompilerParams(vmem_limit_bytes=12 * 1024 * 1024)


def dot(a, b):
    return jnp.dot(a, b, preferred_element_type=f32)


def cost(flops, nbytes):
    return pl.CostEstimate(flops=int(flops), bytes_accessed=int(nbytes), transcendentals=0)


def normalize(output, gain, shift):
    width = output.shape[1]
    mean = jnp.sum(output, axis=1, keepdims=True) * (1.0 / width)
    centered = output - mean
    var = jnp.sum(centered * centered, axis=1, keepdims=True) * (1.0 / width)
    return centered * lax.rsqrt(var + layer_epsilon) * gain + shift


def order_kernel(
    live_ref, send, recv, coarse, halo, after, coarse_out, halo_out, pos_out, code_out, recv_out,
    meta_out, left, right,
):
    h = lax.axis_index("hidden")
    live = live_ref[0]
    rows, lanes = recv.shape
    chunk_bits = (rows * lanes // 4).bit_length() - 1
    number = lax.broadcasted_iota(i32, (rows, lanes), 0) * lanes + lax.broadcasted_iota(
        i32, (rows, lanes), 1
    )
    rel = (lax.shift_right_logical(recv[...], chunk_bits) - h) & 3
    turn = jnp.where(rel == 2, 0, jnp.where(rel == 1, 1, jnp.where(rel == 3, 2, 3)))
    turn = jnp.where(number < live, turn, 4)
    upper = (
        lax.broadcasted_iota(i32, (lanes, lanes), 0) < lax.broadcasted_iota(i32, (lanes, lanes), 1)
    ).astype(f32)
    lower = (
        lax.broadcasted_iota(i32, (rows, rows), 1) < lax.broadcasted_iota(i32, (rows, rows), 0)
    ).astype(f32)
    start = jnp.zeros((1, 1), i32)
    pos = jnp.zeros((rows, lanes), i32)
    lane = lax.broadcasted_iota(i32, (8, 128), 1)
    row8 = lax.broadcasted_iota(i32, (8, 128), 0)
    meta = jnp.zeros((8, 128), i32)
    for v in range(5):
        hit = turn == v
        m = hit.astype(f32)
        within = dot(m, upper)
        above = jnp.sum(dot(lower, m), axis=1, keepdims=True)
        count = jnp.sum(jnp.sum(m, axis=1, keepdims=True), axis=0, keepdims=True).astype(i32)
        pos = jnp.where(hit, start + (within + above).astype(i32), pos)
        meta = jnp.where((row8 == 0) & (lane == v), start, meta)
        meta = jnp.where((row8 == 1) & (lane == v), count, meta)
        start = start + ((count + (BLK - 1)) & ~(BLK - 1))
    far = coarse.shape[1]
    owner = lax.broadcasted_iota(i32, (1, far), 1) // SLOT
    coarse_out[...] = coarse[...] + owner * COARSE_DEV
    halo_out[...] = halo[...] * 4
    pos_out[...] = pos * 4
    slot_rows = code_out.shape[0]
    span = left.shape[0] // 4
    row_number = lax.broadcasted_iota(i32, (span, lanes), 0)
    lane_number = lax.broadcasted_iota(i32, (lanes, lanes), 0)
    for r in range(rows):
        here = pos[r : r + 1, :]
        hit = row_number == lax.shift_right_logical(here, 7)
        code = send[r : r + 1, :]
        target = recv[r : r + 1, :]
        digits = (code & 255, lax.shift_right_logical(code, 8))
        digits += (target & 255, lax.shift_right_logical(target, 8))
        for k, digit in enumerate(digits):
            left[span * k : span * (k + 1), lanes * r : lanes * (r + 1)] = jnp.where(
                hit, digit.astype(f32), 0.0
            ).astype(bf16)
        right[:, lanes * r : lanes * (r + 1)] = (lane_number == (here & (lanes - 1))).astype(bf16)
    sorted_digits = lax.dot_general(
        left[...], right[...], (((1,), (1,)), ((), ())), preferred_element_type=f32
    ).astype(i32)
    low, high = sorted_digits[0:slot_rows], sorted_digits[span : span + slot_rows]
    code_out[...] = (low + high * 256) * 4
    low, high = (sorted_digits[k * span : k * span + slot_rows] for k in (2, 3))
    recv_out[...] = (low + high * 256) * 4
    meta_out[...] = meta


def edge_term_kernel(pos, edges, w, b, after, out, tmp):
    d = w.shape[1]

    def block(i, c):
        base = pl.multiple_of(i * BIG, BIG)
        x = dot(edges[pl.ds(base, BIG), :], w[0:d, :]) + b[...]
        for k in range(4):
            tmp[pl.ds(k, BIG, stride=4), :] = x[:, 128 * k : 128 * (k + 1)]
        for j in range(BIG):
            out[pl.ds(pl.multiple_of(pos[base + j], 4), 4), :] = tmp[4 * j : 4 * j + 4, :]
        return c

    lax.fori_loop(0, edges.shape[0] // BIG, block, 0)


def roll_rows(dst, w, offset, h):
    for k in range(4):
        first = pl.multiple_of(offset + 128 * ((h + k) & 3), 128)
        dst[128 * k : 128 * (k + 1), :] = w[pl.ds(first, 128), :]


def project_kernel(halo, s0, s1, s2a, s2b, s3, w, after, x_out, x_rows, tab, back, forw, tmp, wr):
    n = s0.shape[0]
    half = n // 2
    d = w.shape[1]
    roll_rows(wr, w, d, lax.axis_index("hidden"))
    x_out[:, 0:128] = s0[...]
    x_out[:, 128:256] = s1[...]
    x_out[0:half, 256:384] = s2a[...]
    x_out[half:n, 256:384] = s2b[...]
    x_out[:, 384:512] = s3[...]
    quarter = n // 4
    mine = pl.multiple_of(lax.axis_index("hidden") * quarter, quarter)
    x_rows[...] = x_out[pl.ds(mine, quarter), :]

    def proj(i, c):
        base = pl.multiple_of(i * 512, 512)
        y = dot(x_out[pl.ds(base, 512), :], wr[...])
        for k in range(4):
            tab[pl.ds(base * 4 + k, 512, stride=4), :] = y[:, 128 * k : 128 * (k + 1)]
        return c

    lax.fori_loop(0, n // 512, proj, 0)
    for side, dst in ((0, back), (1, forw)):

        def rows(i, c):
            base = pl.multiple_of(i * BIG, BIG)
            for j in range(BIG):
                r = halo[side * dst.shape[0] + base + j]
                tmp[4 * j : 4 * j + 4, :] = tab[pl.ds(pl.multiple_of(r, 4), 4), :]
            for k in range(4):
                dst[pl.ds(base, BIG), 128 * k : 128 * (k + 1)] = tmp[
                    pl.ds(k, BIG, stride=4), :
                ].astype(bf16)
            return c

        lax.fori_loop(0, back.shape[0] // BIG, rows, 0)


def over_blocks(count, big, small):
    rest = count & (BIG - 1)
    many = (count // BIG) + (rest > BLK).astype(i32)
    lax.fori_loop(0, many, big, 0)

    @pl.when((rest > 0) & (rest <= BLK))
    def _():
        small(many, 0)


def targets(word, s, size):
    row = s // BLK
    if size == BLK:
        both = word[pl.ds(row, 1), :]
    else:
        both = jnp.concatenate([word[pl.ds(row, 1), :], word[pl.ds(row + 1, 1), :]], axis=1)
    return both


def receiver_kernel(x, w, after, tab, wr):
    d = w.shape[1]
    roll_rows(wr, w, 2 * d, lax.axis_index("hidden"))

    def proj(i, c):
        base = pl.multiple_of(i * 512, 512)
        y = dot(x[pl.ds(base, 512), :], wr[...])
        for k in range(4):
            tab[pl.ds(base * 4 + k, 512, stride=4), :] = y[:, 128 * k : 128 * (k + 1)]
        return c

    lax.fori_loop(0, x.shape[0] // 512, proj, 0)


def chunk_messages(v, meta, h, code, recv, words, tab, rtab, term, w, b, gain, shift, msg, tmp, acc):
    quarter = acc.shape[0]
    rel = (2, 1, 3, 0)[v]
    first = ((h + rel) & 3) * quarter
    start = meta[0, v]
    count = meta[1, v]
    acc[...] = jnp.zeros_like(acc)

    def block(size, i, c):
        s = pl.multiple_of(start + i * BIG, BLK)
        for j in range(size):
            sent = tab[pl.ds(pl.multiple_of(code[s + j], 4), 4), :]
            tmp[4 * j : 4 * j + 4, :] = sent + rtab[pl.ds(pl.multiple_of(recv[s + j], 4), 4), :]
        parts = []
        for k in range(4):
            pre = term[pl.ds(s * 4 + k, size, stride=4), :] + tmp[pl.ds(k, size, stride=4), :]
            parts.append((pre / (1.0 + jnp.exp(-pre))).astype(bf16))
        active = jnp.concatenate(parts, axis=1)
        update = normalize(dot(active, w[...]) + b[...], gain[...], shift[...])
        valid = lax.broadcasted_iota(i32, (size, 1), 0) + i * BIG < count
        message = jnp.where(valid, update, 0.0)
        for k in range(4):
            msg[pl.ds(s * 4 + k, size, stride=4), :] = message[:, 128 * k : 128 * (k + 1)]
        target = targets(words, s, size) - first * 4
        hot = (lax.broadcasted_iota(i32, (quarter, size), 0) * 4 == target).astype(bf16)
        acc[...] += dot(hot, message.astype(bf16))
        return c

    over_blocks(count, functools.partial(block, BIG), functools.partial(block, BLK))


def first_kernel(
    meta, code, recv, words, prev, nxt, c0, c1, c2, c3, w_in, rtab, term, w, b, gain, shift, tab_in,
    top, bottom, msg, tab, tmp, acc,
):
    d = w.shape[1]
    border = prev.shape[0]
    far = c0.shape[0]
    n4 = tab.shape[0] - 8 * border - 4 * far
    h = lax.axis_index("hidden")
    for t, src in ((0, prev), (1, nxt)):

        def conv(i, c):
            base = pl.multiple_of(i * 256, 256)
            for k in range(4):
                tab[pl.ds(n4 + t * 4 * border + base * 4 + k, 256, stride=4), :] = src[
                    pl.ds(base, 256), 128 * k : 128 * (k + 1)
                ].astype(f32)
            return c

        lax.fori_loop(0, border // 256, conv, 0)
    y = jnp.zeros((far, d), f32)
    for k, c in enumerate((c0, c1, c2, c3)):
        y = y + dot(c[...], w_in[pl.ds(pl.multiple_of(d + 128 * ((h + k) & 3), 128), 128), :])
    for k in range(4):
        tab[pl.ds(n4 + 8 * border + k, far, stride=4), :] = y[:, 128 * k : 128 * (k + 1)]
    chunk_messages(0, meta, h, code, recv, words, tab, rtab, term, w, b, gain, shift, msg, tmp, acc)
    half = acc.shape[0] // 2
    top[...] = acc[0:half, :].astype(bf16)
    bottom[...] = acc[half:, :].astype(bf16)


def own_kernel(
    meta, code, recv, words, tab, rtab, term, w, b, gain, shift, msg_in, after, sums, msg, tmp, acc
):
    chunk_messages(3, meta, lax.axis_index("hidden"), code, recv, words, tab, rtab, term, w, b, gain, shift, msg, tmp, acc)
    sums[...] = acc[...].astype(bf16)


def near_kernel(
    meta, code, recv, words, tab, rtab, term, w, b, gain, shift, msg_in, up, down, msg, tmp
):
    h = lax.axis_index("hidden")
    for v, acc in ((1, up), (2, down)):
        chunk_messages(
            v, meta, h, code, recv, words, tab, rtab, term, w, b, gain, shift, msg, tmp, acc
        )


def join_kernel(up, down, topgot, bottomgot, up_out, down_out):
    half = topgot.shape[0]
    up_out[0:half, :] = (up[0:half, :] + topgot[...].astype(f32)).astype(bf16)
    up_out[half:, :] = up[half:, :].astype(bf16)
    down_out[0:half, :] = down[0:half, :].astype(bf16)
    down_out[half:, :] = (down[half:, :] + bottomgot[...].astype(f32)).astype(bf16)


def edges_out_kernel(live_ref, pos, edges, msg, out, done, tmp):
    live = live_ref[0]
    done[...] = jnp.zeros_like(done)

    def block(i, c):
        base = pl.multiple_of(i * BIG, BIG)
        for j in range(BIG):
            tmp[4 * j : 4 * j + 4, :] = msg[pl.ds(pl.multiple_of(pos[base + j], 4), 4), :]
        valid = lax.broadcasted_iota(i32, (BIG, 1), 0) + base < live
        for k in range(4):
            old = edges[pl.ds(base, BIG), 128 * k : 128 * (k + 1)].astype(f32)
            add = jnp.where(valid, tmp[pl.ds(k, BIG, stride=4), :], 0.0)
            out[pl.ds(base, BIG), 128 * k : 128 * (k + 1)] = (old + add).astype(bf16)
        return c

    lax.fori_loop(0, edges.shape[0] // BIG, block, 0)


def node_kernel(
    x, own, up, down, w1, b1, w2, b2, gain, shift, after, o0, o1, o2, o3, wr, wc, vec
):
    h = lax.axis_index("hidden")
    d = w2.shape[1]
    quarter = own.shape[0]
    roll_rows(wr, w1, 0, h)
    for k in range(4):
        cols = pl.ds(pl.multiple_of(128 * ((h + k) & 3), 128), 128)
        here = slice(128 * k, 128 * (k + 1))
        wc[:, here] = w2[:, cols]
        vec[0:1, here] = b2[:, cols]
        vec[1:2, here] = gain[:, cols]
        vec[2:3, here] = shift[:, cols]
    half = quarter // 2
    for t in range(2):
        part = slice(t * half, (t + 1) * half)
        total = own[part, :].astype(f32) + up[part, :].astype(f32) + down[part, :].astype(f32)
        mine = x[part, :]
        pre = dot(mine, wr[...]) + dot(total.astype(bf16), w1[d : 2 * d, :]) + b1[...]
        active = (pre / (1.0 + jnp.exp(-pre))).astype(bf16)
        update = normalize(dot(active, wc[...]) + vec[0:1, :], vec[1:2, :], vec[2:3, :])
        new = (mine.astype(f32) + update).astype(bf16)
        for k, o in enumerate((o0, o1, o2, o3)):
            o[part, :] = new[:, 128 * k : 128 * (k + 1)]


def far_rows_kernel(index, everyone, out):
    far = out.shape[0]
    rows = everyone.shape[0]
    hot = lax.broadcasted_iota(i32, (rows, far), 0) == index[...]
    got = lax.dot_general(
        hot.astype(bf16),
        everyone[...],
        (((0,), (0,)), ((), ())),
        preferred_element_type=f32,
    )
    out[...] = got.astype(bf16)


def gather_out_kernel(p0, p1, p2, p3, out):
    quarter = p0.shape[0]
    h = lax.axis_index("hidden")
    for k, p in enumerate((p0, p1, p2, p3)):
        first = pl.multiple_of(((h + k) & 3) * quarter, quarter)
        out[pl.ds(first, quarter), :] = p[...]


def sds(shape, dtype):
    return jax.ShapeDtypeStruct(shape, dtype)


def shifted(array, step):
    n = lax.axis_size("hidden")
    return lax.ppermute(array, "hidden", [(i, (i + step) % n) for i in range(n)])


def chained(array, step):
    n = lax.axis_size("patch")
    return lax.ppermute(array, "patch", [(i, (i + step) % n) for i in range(n)])


def call(kernel, name, out_shape, in_specs, out_specs, scratch=(), flops=1e9, **kw):
    return pl.pallas_call(
        kernel,
        out_shape=out_shape,
        in_specs=in_specs,
        out_specs=out_specs,
        scratch_shapes=list(scratch),
        compiler_params=PARAMS,
        name=name,
        cost_estimate=cost(flops, 4e6),
        **kw,
    )


def local(
    nodes,
    edges,
    senders,
    receivers,
    halo_rows,
    coarse_rows,
    edge_count,
    w_edge_in,
    b_edge_in,
    w_edge_out,
    b_edge_out,
    edge_gain,
    edge_shift,
    w_node_in,
    b_node_in,
    w_node_out,
    b_node_out,
    node_gain,
    node_shift,
):
    n = nodes.shape[0]
    d = edges.shape[1]
    ne = edges.shape[0]
    half = n // 2
    quarter = n // 4
    border = halo_rows.shape[2]
    patches = lax.axis_size("patch")
    slots = ne + 4 * BLK

    up = shifted(nodes, 1)
    down = shifted(nodes, -1)
    farA = shifted(up[:half], 1)
    farB = shifted(down[half:], -1)

    mine = jnp.broadcast_to(nodes[None, :COARSE_DEV], (patches, COARSE_DEV, nodes.shape[1]))
    everyone = lax.all_to_all(mine, "patch", 0, 0, tiled=True).reshape(patches * COARSE_DEV, -1)
    far = coarse_rows.shape[1] * coarse_rows.shape[2]

    row = lambda v: v.reshape(1, -1)
    square = lambda v: v.reshape(ne // 128, 128)
    table = sds((4 * (n + 2 * border + far), 128), f32)
    spread = sds((slots * 4, 128), f32)
    rows_f32 = pltpu.VMEM((4 * BIG, 128), f32)
    weight = pltpu.VMEM((d, d), bf16)
    sums_acc = pltpu.VMEM((quarter, d), f32)

    index, halo4, pos, code, recv, meta = call(
        order_kernel,
        "order",
        (
            sds((1, far), i32),
            sds((2 * border // 128, 128), i32),
            sds((ne // 128, 128), i32),
            sds((slots // 128, 128), i32),
            sds((slots // 128, 128), i32),
            sds((8, 128), i32),
        ),
        [SM] + [VM] * 4 + [ANY],
        (VM,) * 6,
        [pltpu.VMEM((128, ne), bf16), pltpu.VMEM((128, ne), bf16)],
    )(
        edge_count,
        square(senders),
        square(receivers),
        coarse_rows.reshape(1, far),
        halo_rows.reshape(2 * border // 128, 128),
        up,
    )
    pos = pos.reshape(ne)
    c0 = call(far_rows_kernel, "far_rows", sds((far, nodes.shape[1]), bf16), [VM, VM], VM)(
        index, everyone
    )
    c3 = shifted(c0, 1)
    c1 = shifted(c0, -1)
    c2 = shifted(c0, 2)
    pos = pos.reshape(ne)
    x, x_rows, tab, back, forw = call(
        project_kernel,
        "project",
        (
            sds((n, d), bf16),
            sds((quarter, d), bf16),
            table,
            sds((border, d), bf16),
            sds((border, d), bf16),
        ),
        [SM] + [VM] * 6 + [ANY],
        (VM,) * 5,
        [rows_f32, weight],
        flops=6e9,
    )(halo4.reshape(2 * border), nodes, down, farA, farB, up, w_edge_in, c0)
    prev = chained(forw, 1)
    nxt = chained(back, -1)

    term = call(
        edge_term_kernel,
        "edge_term",
        spread,
        [SM, VM, VM, VM, ANY],
        VM,
        [rows_f32],
        flops=6e9,
    )(pos, edges, w_edge_in, row(b_edge_in), x_rows)

    rtab = call(
        receiver_kernel,
        "receiver",
        sds((n * 4, 128), f32),
        [VM, VM, ANY],
        VM,
        [weight],
        flops=3e9,
    )(x, w_edge_in, x_rows)

    layer = (rtab, term, w_edge_out, row(b_edge_out), row(edge_gain), row(edge_shift))
    index_of = (meta, code.reshape(slots), recv.reshape(slots), recv)
    part = sds((quarter // 2, d), bf16)
    whole = sds((quarter, d), bf16)
    whole_f32 = sds((quarter, d), f32)
    top, bottom, msg, tab = call(
        first_kernel,
        "first",
        (part, part, spread, table),
        [SM, SM, SM] + [VM] * 15,
        (VM, VM, VM, VM),
        [rows_f32, sums_acc],
        flops=3e9,
        input_output_aliases={17: 3},
    )(*index_of, prev, nxt, c0, c1, c2, c3, w_edge_in, *layer, tab)
    topgot = shifted(top, 1)
    bottomgot = shifted(bottom, -1)
    upsum, downsum, msg = call(
        near_kernel,
        "near",
        (whole_f32, whole_f32, spread),
        [SM, SM, SM] + [VM] * 9,
        (VM, VM, VM),
        [rows_f32],
        flops=5e9,
        input_output_aliases={11: 2},
    )(*index_of, tab, *layer, msg)
    upsum, downsum = call(join_kernel, "join", (whole, whole), [VM] * 4, (VM, VM))(
        upsum, downsum, topgot, bottomgot
    )
    upgot = shifted(upsum, 1)
    downgot = shifted(downsum, -1)
    own, msg = call(
        own_kernel,
        "own",
        (whole, spread),
        [SM, SM, SM] + [VM] * 9 + [ANY],
        (VM, VM),
        [rows_f32, sums_acc],
        flops=3e9,
        input_output_aliases={11: 1},
    )(*index_of, tab, *layer, msg, upsum)

    edges_out, done = call(
        edges_out_kernel,
        "edges_out",
        (sds((ne, d), bf16), sds((8, 128), f32)),
        [SM, SM, VM, VM],
        (VM, VM),
        [rows_f32],
        flops=5e9,
    )(edge_count, pos, edges, msg)

    share = sds((quarter, 128), bf16)
    o0, o1, o2, o3 = call(
        node_kernel,
        "node",
        (share,) * 4,
        [VM] * 10 + [ANY],
        (VM,) * 4,
        [weight, weight, pltpu.VMEM((8, d), f32)],
    )(
        x_rows,
        own,
        upgot,
        downgot,
        w_node_in,
        row(b_node_in),
        w_node_out,
        row(b_node_out),
        row(node_gain),
        row(node_shift),
        done,
    )
    from_prev = shifted(o1, 1)
    from_next = shifted(o3, -1)
    from_far = shifted(o2, 2)
    nodes_out = call(
        gather_out_kernel, "gather_out", sds((n, 128), bf16), [VM] * 4, VM
    )(o0, from_next, from_far, from_prev)
    return (nodes_out, edges_out)


def solution(mesh):
    return jax.shard_map(
        local,
        mesh=mesh,
        in_specs=(
            P("patch", "hidden"),
            P(("patch", "hidden"), None),
            P(("patch", "hidden")),
            P(("patch", "hidden")),
            P("patch", None, None),
            P("patch", None, None),
            P(("patch", "hidden")),
        )
        + (P(),) * 12,
        out_specs=(P("patch", "hidden"), P(("patch", "hidden"), None)),
        check_vma=False,
    )
```
